32 devices in a mesh: depth: 2 (over y), lat: 16 (over z, x, core).
Axes of the slice: x: 2, y: 2, z: 4, core: 2. Of those that a mesh axis runs over, the one named last changes fastest.
Arguments:
- down_state: bfloat16 [2, 192, 32768], P('depth', None, 'lat'), may hold values from -6 to 6
- up_state: bfloat16 [2, 192, 32768], P('depth', None, 'lat'), may hold values from -6 to 6
- reflectivity: float32 [2, 32768], P('depth', 'lat'), may hold values from -0.3 to 0.3
- w_down: bfloat16 [2, 16, 2048, 1024], P('depth', 'lat'), may hold values from -0.125 to 0.125
- w_up: bfloat16 [2, 16, 2048, 1024], P('depth', 'lat'), may hold values from -0.125 to 0.125
Outputs:
- down_final: bfloat16 [2, 192, 32768], P('depth', None, 'lat')
- up_final: bfloat16 [2, 192, 32768], P('depth', None, 'lat')
The draws below stay inside these ranges and needn't reach their ends.
All inputs are finite; a program needn't handle non-finite values.
Results may differ from the reference program's by a relative error of at most 0.0086.
Values may be sent and summed in bfloat16 or wider, within the bound.
A program may use at most 64 MiB of HBM per device.

```python
import jax
import jax.numpy as jnp
from jax import lax

BLOCK = 1024
HALO = 512
COLS = 192
TICKS = 4
WINDOW = 2048
TILES = 16
LATERAL = 32768
DEPTHS = 2


def level_of(stream_key, dims, pieces, smallest, largest):
    def one(position, shards_of):
        draws = jax.random.uniform(jax.random.fold_in(jax.random.fold_in(stream_key, 6), position), (shards_of,), jnp.float32, smallest / len(pieces), largest / len(pieces))
        return jnp.repeat(jnp.exp(draws), dims[position] // shards_of).reshape((-1,) + (1,) * (len(dims) - position - 1))

    factor_of = one(*pieces[0])
    for cut in pieces[1:]:
        factor_of = factor_of * one(*cut)
    return factor_of


def normal_values(own_key, shape, scale, limit, pieces=(), kind=jnp.bfloat16):
    entries = jax.random.normal(own_key, shape, jnp.float32) * scale
    if len(pieces) > 0:
        entries = level_of(own_key, shape, pieces, -0.22, 0.18) * entries
    return jnp.clip(entries, min=-limit, max=limit).astype(kind)


def setup_inputs(seed: int = 0) -> dict:
    keys = jax.random.split(jax.random.key(seed), 6)
    down_state = normal_values(keys[0], (DEPTHS, COLS, LATERAL), 1.0, 6.0, ((0, 2), (2, 16)))
    up_state = normal_values(keys[1], (DEPTHS, COLS, LATERAL), 1.0, 6.0, ((0, 2), (2, 16)))
    reflectivity = jnp.clip(jax.random.uniform(keys[2], (DEPTHS, LATERAL), jnp.float32, -0.3, 0.3) * level_of(keys[2], (DEPTHS, LATERAL), ((0, 2), (1, 16)), -0.4, 0.0), -0.3, 0.3)
    w_down = normal_values(keys[3], (DEPTHS, TILES, WINDOW, BLOCK), WINDOW ** -0.5, 0.125, ((0, 2), (1, 16)))
    w_up = normal_values(keys[4], (DEPTHS, TILES, WINDOW, BLOCK), WINDOW ** -0.5, 0.125, ((0, 2), (1, 16)))
    return dict(down_state=down_state, up_state=up_state, reflectivity=reflectivity, w_down=w_down, w_up=w_up)


def extrapolate(mixed, weight):
    levels, columns, points = mixed.shape
    block_count = points // BLOCK
    tile_count = weight.shape[1]
    centre_part = mixed.reshape(levels, columns, block_count, BLOCK)
    zero_rim = jnp.zeros((levels, columns, 1, HALO), mixed.dtype)
    left_rim = jnp.concatenate([zero_rim, centre_part[:, :, :-1, BLOCK - HALO:]], axis=2)
    right_rim = jnp.concatenate([centre_part[:, :, 1:, :HALO], zero_rim], axis=2)
    windows = jnp.concatenate([left_rim, centre_part, right_rim], axis=3)
    windows = windows.reshape(levels, columns, tile_count, block_count // tile_count, WINDOW)

    def per_level(operands):
        window_rows, level_weight = operands
        return jnp.einsum("ctbw,two->ctbo", window_rows.astype(jnp.float32), level_weight.astype(jnp.float32), precision=lax.Precision.HIGHEST)

    product = lax.map(per_level, (windows, weight))
    return product.reshape(levels, columns, points)


def reference(down_state, up_state, reflectivity, w_down, w_up):
    reflect_col = reflectivity[:, None, :]
    going_down, going_up = down_state, up_state
    for tick_index in range(TICKS):
        down_wide = going_down.astype(jnp.float32)
        up_wide = going_up.astype(jnp.float32)
        mixed_down = ((1.0 + reflect_col) * down_wide - reflect_col * up_wide).astype(jnp.bfloat16)
        mixed_up = ((1.0 - reflect_col) * up_wide + reflect_col * down_wide).astype(jnp.bfloat16)
        out_down = extrapolate(mixed_down, w_down).astype(jnp.bfloat16)
        out_up = extrapolate(mixed_up, w_up).astype(jnp.bfloat16)
        going_down = jnp.concatenate([-out_up[:1], out_down[:-1]], axis=0)
        going_up = jnp.concatenate([out_up[1:], jnp.zeros_like(out_up[:1])], axis=0)
    return going_down, going_up
```

```python
import functools

import jax
import jax.numpy as jnp
from jax import lax
from jax.experimental import pallas as pl
from jax.experimental.pallas import tpu as pltpu
from jax.sharding import PartitionSpec as P

BLOCK = 1024
HALO = 512
TICKS = 4
SLICE = 256
SLICES = BLOCK // SLICE
VMEM_BYTES = 67043328
MESH = pl.DeviceIdType.MESH


def chunks_of(columns):
    for count in (3, 2):
        if columns % (16 * count) == 0:
            return count
    return 1


def kernel(
    depths, lats, chunks,
    down_in, up_in, reflect_in, wd_in, wu_in,
    down_out, up_out,
    state, padded, outs, weights, reflect_ref,
    in_sem, w_sem, r_sem, halo_send, halo_recv, depth_send, depth_recv,
):
    level = lax.axis_index("depth")
    lat = lax.axis_index("lat")
    rows, points = state.shape[2], state.shape[3]
    steps = TICKS * chunks
    blocks = points // BLOCK
    not_first, not_last = level > 0, level < depths - 1
    has_left, has_right = lat > 0, lat < lats - 1
    neighbours = (
        (has_left, {"lat": lat - 1}),
        (has_right, {"lat": lat + 1}),
        (not_first, {"depth": level - 1}),
        (not_last, {"depth": level + 1}),
    )

    def in_copy(c, f):
        source = (down_in, up_in)[f]
        return pltpu.make_async_copy(
            source.at[0, pl.ds(c * rows, rows)], state.at[c, f], in_sem.at[c, f]
        )

    def w_copy(f, n):
        columns = pl.ds(pl.multiple_of(n * SLICE, SLICE), SLICE)
        return pltpu.make_async_copy(
            (wd_in, wu_in)[f].at[0, 0, :, columns], weights.at[f, :, columns], w_sem.at[f, n]
        )

    def weights_wait(f, n):
        for g in range(2):
            @pl.when(f == g)
            def _():
                w_copy(g, n).wait()

    def r_copy():
        return pltpu.make_async_copy(reflect_in, reflect_ref, r_sem)

    def halo_copy(k, side, f):
        source = HALO if side == 0 else points
        target = HALO + points if side == 0 else 0
        return pltpu.make_async_remote_copy(
            src_ref=padded.at[k, f, :, pl.ds(source, HALO)],
            dst_ref=padded.at[k, f, :, pl.ds(target, HALO)],
            send_sem=halo_send.at[k, side, f],
            recv_sem=halo_recv.at[k, side, f],
            device_id={"lat": lat - 1 if side == 0 else lat + 1},
            device_id_type=MESH,
        )

    def next_state(k, f, last):
        if last:
            start = pl.multiple_of((k - (steps - chunks)) * rows, rows)
            return (down_out, up_out)[f].at[0, pl.ds(start, rows)]
        return state.at[k + chunks, f]

    def depth_copy(k, f, last):
        return pltpu.make_async_remote_copy(
            src_ref=outs.at[k, f],
            dst_ref=next_state(k, f, last),
            send_sem=depth_send.at[k, f],
            recv_sem=depth_recv.at[k, f],
            device_id={"depth": level + 1 if f == 0 else level - 1},
            device_id_type=MESH,
        )

    def depth_slice(k, f, start):
        columns = pl.ds(start, SLICE)
        return pltpu.make_async_remote_copy(
            src_ref=outs.at[k, f, :, columns],
            dst_ref=next_state(k, f, False).at[:, columns],
            send_sem=depth_send.at[k, f],
            recv_sem=depth_recv.at[k, f],
            device_id={"depth": level + 1 if f == 0 else level - 1},
            device_id_type=MESH,
        )

    def in_turn(turn):
        return lax.rem(turn + (level == depths - 1).astype(jnp.int32), 2)

    barrier = pltpu.get_barrier_semaphore()
    for present, device in neighbours:
        @pl.when(present)
        def _():
            pl.semaphore_signal(barrier, inc=1, device_id=device, device_id_type=MESH)

    for f in range(2):
        in_copy(0, f).start()
    r_copy().start()
    def weights_start(f, n):
        for g in range(2):
            @pl.when(f == g)
            def _():
                w_copy(g, n).start()

    def arrived(k, last):
        @pl.when(not_first)
        def _():
            depth_copy(k, 0, last).wait_recv()

        @pl.when(not_last)
        def _():
            depth_copy(k, 1, last).wait_recv()

    def mix_field(k, f):
        reflect = jnp.where(f == 0, 1.0, -1.0) * reflect_ref[...]
        own = state[k, f].astype(jnp.float32)
        other = state[k, 1 - f].astype(jnp.float32)
        padded[k, f, :, HALO : HALO + points] = (
            (1.0 + reflect) * own - reflect * other
        ).astype(jnp.bfloat16)

    def send_halo(k, f):
        @pl.when(has_left)
        def _():
            halo_copy(k, 0, f).start()

        @pl.when(has_right)
        def _():
            halo_copy(k, 1, f).start()

    def mix(k):
        @pl.loop(0, 2)
        def _(turn):
            f = in_turn(turn)
            mix_field(k, f)
            send_halo(k, f)

    def finish(k, f, last):
        @pl.when((f == 1) & (level == 0))
        def _():
            next_state(k, 0, last)[...] = -outs[k, 1]

        @pl.when((f == 1) & (level == depths - 1))
        def _():
            next_state(k, 1, last)[...] = jnp.zeros((rows, points), jnp.bfloat16)

    def first_block(f, b):
        rim = b == blocks - 1

        @pl.when(rim & has_right)
        def _():
            halo_copy(0, 0, f).wait_recv()

        @pl.when((b == 0) & has_left)
        def _():
            halo_copy(0, 1, f).wait_recv()

        @pl.loop(0, SLICES)
        def _(n):
            @pl.when(b == near)
            def _():
                weights_wait(f, n)

            base = pl.multiple_of(b * BLOCK, BLOCK)
            start = pl.multiple_of(base + n * SLICE, SLICE)
            columns = pl.ds(pl.multiple_of(n * SLICE, SLICE), SLICE)
            outs[0, f, :, pl.ds(start, SLICE)] = jnp.dot(
                padded[0, f, :, pl.ds(base, BLOCK + 2 * HALO)],
                weights[f, :, columns],
                preferred_element_type=jnp.float32,
            ).astype(jnp.bfloat16)

            @pl.when((f == 0) & not_last)
            def _():
                depth_slice(0, 0, start).start()

            @pl.when((f == 1) & not_first)
            def _():
                depth_slice(0, 1, start).start()

    def extrapolate_field(k, f, last):
        @pl.when(has_right)
        def _():
            halo_copy(k, 0, f).wait_recv()

        @pl.when(has_left)
        def _():
            halo_copy(k, 1, f).wait_recv()

        windows = jnp.concatenate(
            [padded[k, f, :, b * BLOCK : b * BLOCK + BLOCK + 2 * HALO] for b in range(blocks)],
            axis=0,
        )
        summed = jnp.dot(windows, weights[f], preferred_element_type=jnp.float32)
        summed = summed.astype(jnp.bfloat16)
        for b in range(blocks):
            outs[k, f, :, b * BLOCK : (b + 1) * BLOCK] = summed[b * rows : (b + 1) * rows]

        @pl.when((f == 0) & not_last)
        def _():
            depth_copy(k, 0, last).start()

        @pl.when((f == 1) & not_first)
        def _():
            depth_copy(k, 1, last).start()

        finish(k, f, last)

    def extrapolate(k, last):
        @pl.loop(0, 2)
        def _(turn):
            extrapolate_field(k, in_turn(turn), last)

    zero_rim = jnp.zeros((2, rows, HALO), jnp.bfloat16)

    @pl.when(lat == 0)
    def _():
        @pl.loop(0, steps)
        def _(k):
            padded[k, :, :, :HALO] = zero_rim

    @pl.when(lat == lats - 1)
    def _():
        @pl.loop(0, steps)
        def _(k):
            padded[k, :, :, HALO + points :] = zero_rim

    early, late = in_turn(0), in_turn(1)
    near = lax.rem(lat + 1, 2)
    for f in range(2):
        in_copy(0, f).wait()
    r_copy().wait()
    weights_start(early, 0)
    weights_start(early, 1)
    mix_field(0, early)
    pl.semaphore_wait(barrier, sum(present.astype(jnp.int32) for present, _ in neighbours))
    send_halo(0, early)
    for n in range(2, SLICES):
        weights_start(early, n)
    mix_field(0, late)
    send_halo(0, late)
    for f in range(2):
        in_copy(1, f).start()

    first_block(early, near)
    for n in range(SLICES):
        weights_start(late, n)
    for c in range(2, chunks):
        for f in range(2):
            in_copy(c, f).start()
    for f in range(2):
        in_copy(1, f).wait()
    mix(1)
    first_block(early, 1 - near)
    finish(0, early, False)
    for n in range(SLICES):
        weights_wait(late, n)
    extrapolate_field(0, late, False)

    for c in range(2, chunks):
        for f in range(2):
            in_copy(c, f).wait()

    @pl.loop(2, chunks)
    def _(k):
        mix(k)

    @pl.loop(1, chunks - 1)
    def _(k):
        extrapolate(k, False)

    @pl.loop(chunks, steps - chunks + 1)
    def _(k):
        arrived(k - chunks, False)
        mix(k)
        extrapolate(k - 1, False)

    @pl.loop(steps - chunks + 1, steps)
    def _(k):
        arrived(k - chunks, False)
        mix(k)
        extrapolate(k - 1, True)

    extrapolate(steps - 1, True)

    def sent(k, last):
        for f in range(2):
            @pl.when(has_left)
            def _():
                halo_copy(k, 0, f).wait_send()

            @pl.when(has_right)
            def _():
                halo_copy(k, 1, f).wait_send()

        @pl.when(not_last)
        def _():
            depth_copy(k, 0, last).wait_send()

        @pl.when(not_first)
        def _():
            depth_copy(k, 1, last).wait_send()

    @pl.loop(0, steps - chunks)
    def _(k):
        sent(k, False)

    @pl.loop(steps - chunks, steps)
    def _(k):
        sent(k, True)
        arrived(k, True)


def solution(mesh):
    depths, lats = mesh.shape["depth"], mesh.shape["lat"]

    def on_device(down_state, up_state, reflectivity, w_down, w_up):
        _, columns, points = down_state.shape
        chunks = chunks_of(columns)
        rows = columns // chunks
        steps = TICKS * chunks
        window = w_down.shape[2]
        field = pltpu.VMEM(down_state.shape, jnp.bfloat16)
        landing = pl.BlockSpec(memory_space=pltpu.VMEM)
        anywhere = pl.BlockSpec(memory_space=pl.ANY)
        flops = 2 * 2 * TICKS * columns * points * window
        return pl.pallas_call(
            functools.partial(kernel, depths, lats, chunks),
            out_shape=(field, field),
            in_specs=[anywhere] * 5,
            out_specs=(landing, landing),
            scratch_shapes=[
                pltpu.VMEM((steps, 2, rows, points), jnp.bfloat16),
                pltpu.VMEM((steps, 2, rows, points + 2 * HALO), jnp.bfloat16),
                pltpu.VMEM((steps, 2, rows, points), jnp.bfloat16),
                pltpu.VMEM((2, window, BLOCK), jnp.bfloat16),
                pltpu.VMEM((1, points), jnp.float32),
                pltpu.SemaphoreType.DMA((chunks, 2)),
                pltpu.SemaphoreType.DMA((2, SLICES)),
                pltpu.SemaphoreType.DMA,
                pltpu.SemaphoreType.DMA((steps, 2, 2)),
                pltpu.SemaphoreType.DMA((steps, 2, 2)),
                pltpu.SemaphoreType.DMA((steps, 2)),
                pltpu.SemaphoreType.DMA((steps, 2)),
            ],
            compiler_params=pltpu.CompilerParams(
                collective_id=0, has_side_effects=True, vmem_limit_bytes=VMEM_BYTES - 2 * 2 * down_state.size
            ),
            cost_estimate=pl.CostEstimate(
                flops=flops, bytes_accessed=4 * w_down.size * 2, transcendentals=0
            ),
        )(down_state, up_state, reflectivity, w_down, w_up)

    in_specs = (
        P("depth", None, "lat"),
        P("depth", None, "lat"),
        P("depth", "lat"),
        P("depth", "lat", None, None),
        P("depth", "lat", None, None),
    )
    out_specs = (P("depth", None, "lat"), P("depth", None, "lat"))
    return jax.shard_map(
        on_device, mesh=mesh, in_specs=in_specs, out_specs=out_specs, check_vma=False
    )
```

```python
import functools

import jax
import jax.numpy as jnp
from jax import lax
from jax.experimental import pallas as pl
from jax.experimental.pallas import tpu as pltpu
from jax.sharding import PartitionSpec as P

BLOCK = 1024
HALO = 512
TICKS = 4
SLICE = 256
SLICES = BLOCK // SLICE
VMEM_BYTES = 67043328
MESH = pl.DeviceIdType.MESH


def chunks_of(columns):
    for count in (3, 2):
        if columns % (16 * count) == 0:
            return count
    return 1


def kernel(
    depths, lats, chunks,
    down_in, up_in, reflect_in, wd_in, wu_in,
    down_out, up_out,
    state, padded, outs, weights, reflect_ref,
    in_sem, w_sem, r_sem, halo_send, halo_recv, depth_send, depth_recv,
):
    level = lax.axis_index("depth")
    lat = lax.axis_index("lat")
    rows, points = state.shape[2], state.shape[3]
    steps = TICKS * chunks
    blocks = points // BLOCK
    not_first, not_last = level > 0, level < depths - 1
    has_left, has_right = lat > 0, lat < lats - 1
    neighbours = (
        (has_left, {"lat": lat - 1}),
        (has_right, {"lat": lat + 1}),
        (not_first, {"depth": level - 1}),
        (not_last, {"depth": level + 1}),
    )

    def in_copy(c, f):
        source = (down_in, up_in)[f]
        return pltpu.make_async_copy(
            source.at[0, pl.ds(c * rows, rows)], state.at[c, f], in_sem.at[c, f]
        )

    def w_copy(f, n):
        columns = pl.ds(pl.multiple_of(n * SLICE, SLICE), SLICE)
        return pltpu.make_async_copy(
            (wd_in, wu_in)[f].at[0, 0, :, columns], weights.at[f, :, columns], w_sem.at[f, n]
        )

    def weights_wait(f, n):
        for g in range(2):
            @pl.when(f == g)
            def _():
                w_copy(g, n).wait()

    def r_copy():
        return pltpu.make_async_copy(reflect_in, reflect_ref, r_sem)

    def halo_copy(k, side, f):
        source = HALO if side == 0 else points
        target = HALO + points if side == 0 else 0
        return pltpu.make_async_remote_copy(
            src_ref=padded.at[k, f, :, pl.ds(source, HALO)],
            dst_ref=padded.at[k, f, :, pl.ds(target, HALO)],
            send_sem=halo_send.at[k, side, f],
            recv_sem=halo_recv.at[k, side, f],
            device_id={"lat": lat - 1 if side == 0 else lat + 1},
            device_id_type=MESH,
        )

    def next_state(k, f, last):
        if last:
            start = pl.multiple_of((k - (steps - chunks)) * rows, rows)
            return (down_out, up_out)[f].at[0, pl.ds(start, rows)]
        return state.at[k + chunks, f]

    def depth_copy(k, f, last):
        return pltpu.make_async_remote_copy(
            src_ref=outs.at[k, f],
            dst_ref=next_state(k, f, last),
            send_sem=depth_send.at[k, f],
            recv_sem=depth_recv.at[k, f],
            device_id={"depth": level + 1 if f == 0 else level - 1},
            device_id_type=MESH,
        )

    def depth_slice(k, f, start):
        columns = pl.ds(start, SLICE)
        return pltpu.make_async_remote_copy(
            src_ref=outs.at[k, f, :, columns],
            dst_ref=next_state(k, f, False).at[:, columns],
            send_sem=depth_send.at[k, f],
            recv_sem=depth_recv.at[k, f],
            device_id={"depth": level + 1 if f == 0 else level - 1},
            device_id_type=MESH,
        )

    def in_turn(turn):
        return lax.rem(turn + (level == depths - 1).astype(jnp.int32), 2)

    barrier = pltpu.get_barrier_semaphore()
    for present, device in neighbours:
        @pl.when(present)
        def _():
            pl.semaphore_signal(barrier, inc=1, device_id=device, device_id_type=MESH)

    for c in range(2):
        for f in range(2):
            in_copy(c, f).start()
    r_copy().start()
    def weights_start(f, n):
        for g in range(2):
            @pl.when(f == g)
            def _():
                w_copy(g, n).start()

    weights_start(in_turn(0), 0)

    def arrived(k, last):
        @pl.when(not_first)
        def _():
            depth_copy(k, 0, last).wait_recv()

        @pl.when(not_last)
        def _():
            depth_copy(k, 1, last).wait_recv()

    def mix_field(k, f):
        reflect = jnp.where(f == 0, 1.0, -1.0) * reflect_ref[...]
        own = state[k, f].astype(jnp.float32)
        other = state[k, 1 - f].astype(jnp.float32)
        padded[k, f, :, HALO : HALO + points] = (
            (1.0 + reflect) * own - reflect * other
        ).astype(jnp.bfloat16)

    def send_halo(k, f):
        @pl.when(has_left)
        def _():
            halo_copy(k, 0, f).start()

        @pl.when(has_right)
        def _():
            halo_copy(k, 1, f).start()

    def mix(k):
        @pl.loop(0, 2)
        def _(turn):
            f = in_turn(turn)
            mix_field(k, f)
            send_halo(k, f)

    def finish(k, f, last):
        @pl.when((f == 1) & (level == 0))
        def _():
            next_state(k, 0, last)[...] = -outs[k, 1]

        @pl.when((f == 1) & (level == depths - 1))
        def _():
            next_state(k, 1, last)[...] = jnp.zeros((rows, points), jnp.bfloat16)

    def first_block(f, b):
        rim = b == blocks - 1

        @pl.when(rim & has_right)
        def _():
            halo_copy(0, 0, f).wait_recv()

        @pl.when((b == 0) & has_left)
        def _():
            halo_copy(0, 1, f).wait_recv()

        @pl.loop(0, SLICES)
        def _(n):
            @pl.when(b == near)
            def _():
                weights_wait(f, n)

            base = pl.multiple_of(b * BLOCK, BLOCK)
            start = pl.multiple_of(base + n * SLICE, SLICE)
            columns = pl.ds(pl.multiple_of(n * SLICE, SLICE), SLICE)
            outs[0, f, :, pl.ds(start, SLICE)] = jnp.dot(
                padded[0, f, :, pl.ds(base, BLOCK + 2 * HALO)],
                weights[f, :, columns],
                preferred_element_type=jnp.float32,
            ).astype(jnp.bfloat16)

            @pl.when((f == 0) & not_last)
            def _():
                depth_slice(0, 0, start).start()

            @pl.when((f == 1) & not_first)
            def _():
                depth_slice(0, 1, start).start()

    def extrapolate_field(k, f, last):
        @pl.when(has_right)
        def _():
            halo_copy(k, 0, f).wait_recv()

        @pl.when(has_left)
        def _():
            halo_copy(k, 1, f).wait_recv()

        windows = jnp.concatenate(
            [padded[k, f, :, b * BLOCK : b * BLOCK + BLOCK + 2 * HALO] for b in range(blocks)],
            axis=0,
        )
        summed = jnp.dot(windows, weights[f], preferred_element_type=jnp.float32)
        summed = summed.astype(jnp.bfloat16)
        for b in range(blocks):
            outs[k, f, :, b * BLOCK : (b + 1) * BLOCK] = summed[b * rows : (b + 1) * rows]

        @pl.when((f == 0) & not_last)
        def _():
            depth_copy(k, 0, last).start()

        @pl.when((f == 1) & not_first)
        def _():
            depth_copy(k, 1, last).start()

        finish(k, f, last)

    def extrapolate(k, last):
        @pl.loop(0, 2)
        def _(turn):
            extrapolate_field(k, in_turn(turn), last)

    zero_rim = jnp.zeros((2, rows, HALO), jnp.bfloat16)

    @pl.when(lat == 0)
    def _():
        @pl.loop(0, steps)
        def _(k):
            padded[k, :, :, :HALO] = zero_rim

    @pl.when(lat == lats - 1)
    def _():
        @pl.loop(0, steps)
        def _(k):
            padded[k, :, :, HALO + points :] = zero_rim

    early, late = in_turn(0), in_turn(1)
    near = lax.rem(lat + 1, 2)

    def prepare(k, f):
        mix_field(k, f)
        send_halo(k, f)

    def inputs_start(c):
        for f in range(2):
            in_copy(c, f).start()

    def inputs_wait(c):
        for f in range(2):
            in_copy(c, f).wait()

    inputs_wait(0)
    r_copy().wait()
    weights_start(early, 1)
    mix_field(0, early)
    pl.semaphore_wait(barrier, sum(present.astype(jnp.int32) for present, _ in neighbours))
    send_halo(0, early)
    for n in range(2, SLICES):
        weights_start(early, n)
    prepare(0, late)
    for c in range(2, chunks):
        inputs_start(c)
    first_block(early, near)
    for n in range(SLICES):
        weights_start(late, n)
    inputs_wait(1)
    prepare(1, early)
    prepare(1, late)
    for c in range(2, chunks):
        inputs_wait(c)

    @pl.loop(2, chunks)
    def _(k):
        mix(k)

    first_block(early, 1 - near)
    finish(0, early, False)

    @pl.loop(1, chunks - 1)
    def _(k):
        extrapolate_field(k, early, False)

    for n in range(SLICES):
        weights_wait(late, n)

    @pl.loop(0, chunks - 1)
    def _(k):
        extrapolate_field(k, late, False)

    @pl.loop(chunks, steps - chunks + 1)
    def _(k):
        arrived(k - chunks, False)
        mix(k)
        extrapolate(k - 1, False)

    @pl.loop(steps - chunks + 1, steps)
    def _(k):
        arrived(k - chunks, False)
        mix(k)
        extrapolate(k - 1, True)

    extrapolate(steps - 1, True)

    def sent(k, last):
        for f in range(2):
            @pl.when(has_left)
            def _():
                halo_copy(k, 0, f).wait_send()

            @pl.when(has_right)
            def _():
                halo_copy(k, 1, f).wait_send()

        @pl.when(not_last)
        def _():
            depth_copy(k, 0, last).wait_send()

        @pl.when(not_first)
        def _():
            depth_copy(k, 1, last).wait_send()

    @pl.loop(0, steps - chunks)
    def _(k):
        sent(k, False)

    @pl.loop(steps - chunks, steps)
    def _(k):
        sent(k, True)
        arrived(k, True)


def store(down, up, down_out, up_out, sem):
    copies = [
        pltpu.make_async_copy(source, target, sem.at[f])
        for f, (source, target) in enumerate(((down, down_out), (up, up_out)))
    ]
    for copy in copies:
        copy.start()
    for copy in copies:
        copy.wait()


def solution(mesh):
    depths, lats = mesh.shape["depth"], mesh.shape["lat"]

    def on_device(down_state, up_state, reflectivity, w_down, w_up):
        _, columns, points = down_state.shape
        chunks = chunks_of(columns)
        rows = columns // chunks
        steps = TICKS * chunks
        window = w_down.shape[2]
        field = pltpu.VMEM(down_state.shape, jnp.bfloat16)
        landing = pl.BlockSpec(memory_space=pltpu.VMEM)
        anywhere = pl.BlockSpec(memory_space=pl.ANY)
        flops = 2 * 2 * TICKS * columns * points * window
        results = pl.pallas_call(
            functools.partial(kernel, depths, lats, chunks),
            out_shape=(field, field),
            in_specs=[anywhere] * 5,
            out_specs=(landing, landing),
            scratch_shapes=[
                pltpu.VMEM((steps, 2, rows, points), jnp.bfloat16),
                pltpu.VMEM((steps, 2, rows, points + 2 * HALO), jnp.bfloat16),
                pltpu.VMEM((steps, 2, rows, points), jnp.bfloat16),
                pltpu.VMEM((2, window, BLOCK), jnp.bfloat16),
                pltpu.VMEM((1, points), jnp.float32),
                pltpu.SemaphoreType.DMA((chunks, 2)),
                pltpu.SemaphoreType.DMA((2, SLICES)),
                pltpu.SemaphoreType.DMA,
                pltpu.SemaphoreType.DMA((steps, 2, 2)),
                pltpu.SemaphoreType.DMA((steps, 2, 2)),
                pltpu.SemaphoreType.DMA((steps, 2)),
                pltpu.SemaphoreType.DMA((steps, 2)),
            ],
            compiler_params=pltpu.CompilerParams(
                collective_id=0, has_side_effects=True, vmem_limit_bytes=VMEM_BYTES - 2 * 2 * down_state.size
            ),
            cost_estimate=pl.CostEstimate(
                flops=flops, bytes_accessed=4 * w_down.size * 2, transcendentals=0
            ),
        )(down_state, up_state, reflectivity, w_down, w_up)
        results = [pltpu.with_memory_space_constraint(result, pltpu.VMEM) for result in results]
        whole = jax.ShapeDtypeStruct(down_state.shape, jnp.bfloat16)
        return pl.pallas_call(
            store,
            out_shape=(whole, whole),
            in_specs=[landing] * 2,
            out_specs=(anywhere, anywhere),
            scratch_shapes=[pltpu.SemaphoreType.DMA((2,))],
            cost_estimate=pl.CostEstimate(
                flops=0, bytes_accessed=4 * 2 * down_state.size, transcendentals=0
            ),
        )(*results)

    in_specs = (
        P("depth", None, "lat"),
        P("depth", None, "lat"),
        P("depth", "lat"),
        P("depth", "lat", None, None),
        P("depth", "lat", None, None),
    )
    out_specs = (P("depth", None, "lat"), P("depth", None, "lat"))
    return jax.shard_map(
        on_device, mesh=mesh, in_specs=in_specs, out_specs=out_specs, check_vma=False
    )
```

```python
import functools

import jax
import jax.numpy as jnp
from jax import lax
from jax.experimental import pallas as pl
from jax.experimental.pallas import tpu as pltpu
from jax.sharding import PartitionSpec as P

BLOCK = 1024
HALO = 512
TICKS = 4
SLICE = 256
SLICES = BLOCK // SLICE
VMEM_BYTES = 67043328
MESH = pl.DeviceIdType.MESH


def chunks_of(columns):
    for count in (3, 2):
        if columns % (16 * count) == 0:
            return count
    return 1


def kernel(
    depths, lats, chunks,
    down_in, up_in, reflect_in, wd_in, wu_in,
    down_out, up_out,
    state, padded, outs, weights, reflect_ref,
    in_sem, w_sem, r_sem, halo_send, halo_recv, depth_send, depth_recv,
):
    level = lax.axis_index("depth")
    lat = lax.axis_index("lat")
    rows, points = state.shape[2], state.shape[3]
    steps = TICKS * chunks
    ring = 2 * chunks
    blocks = points // BLOCK
    not_first, not_last = level > 0, level < depths - 1
    has_left, has_right = lat > 0, lat < lats - 1
    neighbours = (
        (has_left, {"lat": lat - 1}),
        (has_right, {"lat": lat + 1}),
        (not_first, {"depth": level - 1}),
        (not_last, {"depth": level + 1}),
    )

    def slot(k):
        return k % ring if isinstance(k, int) else lax.rem(k, ring)

    def in_copy(c, f):
        source = (down_in, up_in)[f]
        return pltpu.make_async_copy(
            source.at[0, pl.ds(c * rows, rows)], state.at[c, f], in_sem.at[c, f]
        )

    def w_copy(f, n):
        columns = pl.ds(pl.multiple_of(n * SLICE, SLICE), SLICE)
        return pltpu.make_async_copy(
            (wd_in, wu_in)[f].at[0, 0, :, columns], weights.at[f, :, columns], w_sem.at[f, n]
        )

    def weights_wait(f, n):
        for g in range(2):
            @pl.when(f == g)
            def _():
                w_copy(g, n).wait()

    def r_copy():
        return pltpu.make_async_copy(reflect_in, reflect_ref, r_sem)

    def halo_copy(k, side, f):
        source = HALO if side == 0 else points
        target = HALO + points if side == 0 else 0
        return pltpu.make_async_remote_copy(
            src_ref=padded.at[k, f, :, pl.ds(source, HALO)],
            dst_ref=padded.at[k, f, :, pl.ds(target, HALO)],
            send_sem=halo_send.at[slot(k), side, f],
            recv_sem=halo_recv.at[slot(k), side, f],
            device_id={"lat": lat - 1 if side == 0 else lat + 1},
            device_id_type=MESH,
        )

    def next_state(k, f, last):
        if last:
            start = pl.multiple_of((k - (steps - chunks)) * rows, rows)
            return (down_out, up_out)[f].at[0, pl.ds(start, rows)]
        return state.at[k + chunks, f]

    def depth_copy(k, f, last):
        return pltpu.make_async_remote_copy(
            src_ref=outs.at[k, f],
            dst_ref=next_state(k, f, last),
            send_sem=depth_send.at[slot(k), f],
            recv_sem=depth_recv.at[slot(k), f],
            device_id={"depth": level + 1 if f == 0 else level - 1},
            device_id_type=MESH,
        )

    def depth_slice(k, f, start):
        columns = pl.ds(start, SLICE)
        return pltpu.make_async_remote_copy(
            src_ref=outs.at[k, f, :, columns],
            dst_ref=next_state(k, f, False).at[:, columns],
            send_sem=depth_send.at[slot(k), f],
            recv_sem=depth_recv.at[slot(k), f],
            device_id={"depth": level + 1 if f == 0 else level - 1},
            device_id_type=MESH,
        )

    def in_turn(turn):
        return lax.rem(turn + (level == depths - 1).astype(jnp.int32), 2)

    barrier = pltpu.get_barrier_semaphore()
    for present, device in neighbours:
        @pl.when(present)
        def _():
            pl.semaphore_signal(barrier, inc=1, device_id=device, device_id_type=MESH)

    for c in range(2):
        for f in range(2):
            in_copy(c, f).start()
    r_copy().start()
    def weights_start(f, n):
        for g in range(2):
            @pl.when(f == g)
            def _():
                w_copy(g, n).start()

    weights_start(in_turn(0), 0)

    def arrived(k, last):
        @pl.when(not_first)
        def _():
            depth_copy(k, 0, last).wait_recv()

        @pl.when(not_last)
        def _():
            depth_copy(k, 1, last).wait_recv()

    def mix_field(k, f):
        reflect = jnp.where(f == 0, 1.0, -1.0) * reflect_ref[...]
        own = state[k, f].astype(jnp.float32)
        other = state[k, 1 - f].astype(jnp.float32)
        padded[k, f, :, HALO : HALO + points] = (
            (1.0 + reflect) * own - reflect * other
        ).astype(jnp.bfloat16)

    def send_halo(k, f):
        @pl.when(has_left)
        def _():
            halo_copy(k, 0, f).start()

        @pl.when(has_right)
        def _():
            halo_copy(k, 1, f).start()

    def mix(k):
        @pl.loop(0, 2)
        def _(turn):
            f = in_turn(turn)
            mix_field(k, f)
            send_halo(k, f)

    def finish(k, f, last):
        @pl.when((f == 1) & (level == 0))
        def _():
            next_state(k, 0, last)[...] = -outs[k, 1]

        @pl.when((f == 1) & (level == depths - 1))
        def _():
            next_state(k, 1, last)[...] = jnp.zeros((rows, points), jnp.bfloat16)

    def first_block(f, b):
        rim = b == blocks - 1

        @pl.when(rim & has_right)
        def _():
            halo_copy(0, 0, f).wait_recv()

        @pl.when((b == 0) & has_left)
        def _():
            halo_copy(0, 1, f).wait_recv()

        @pl.loop(0, SLICES)
        def _(n):
            @pl.when(b == near)
            def _():
                weights_wait(f, n)

            base = pl.multiple_of(b * BLOCK, BLOCK)
            start = pl.multiple_of(base + n * SLICE, SLICE)
            columns = pl.ds(pl.multiple_of(n * SLICE, SLICE), SLICE)
            outs[0, f, :, pl.ds(start, SLICE)] = jnp.dot(
                padded[0, f, :, pl.ds(base, BLOCK + 2 * HALO)],
                weights[f, :, columns],
                preferred_element_type=jnp.float32,
            ).astype(jnp.bfloat16)

            @pl.when((f == 0) & not_last)
            def _():
                depth_slice(0, 0, start).start()

            @pl.when((f == 1) & not_first)
            def _():
                depth_slice(0, 1, start).start()

    def extrapolate_field(k, f, last):
        @pl.when(has_right)
        def _():
            halo_copy(k, 0, f).wait_recv()

        @pl.when(has_left)
        def _():
            halo_copy(k, 1, f).wait_recv()

        windows = jnp.concatenate(
            [padded[k, f, :, b * BLOCK : b * BLOCK + BLOCK + 2 * HALO] for b in range(blocks)],
            axis=0,
        )
        summed = jnp.dot(windows, weights[f], preferred_element_type=jnp.float32)
        summed = summed.astype(jnp.bfloat16)
        for b in range(blocks):
            outs[k, f, :, b * BLOCK : (b + 1) * BLOCK] = summed[b * rows : (b + 1) * rows]

        @pl.when((f == 0) & not_last)
        def _():
            depth_copy(k, 0, last).start()

        @pl.when((f == 1) & not_first)
        def _():
            depth_copy(k, 1, last).start()

        finish(k, f, last)

    def extrapolate(k, last):
        @pl.loop(0, 2)
        def _(turn):
            extrapolate_field(k, in_turn(turn), last)

    zero_rim = jnp.zeros((2, rows, HALO), jnp.bfloat16)

    @pl.when(lat == 0)
    def _():
        @pl.loop(0, steps)
        def _(k):
            padded[k, :, :, :HALO] = zero_rim

    @pl.when(lat == lats - 1)
    def _():
        @pl.loop(0, steps)
        def _(k):
            padded[k, :, :, HALO + points :] = zero_rim

    early, late = in_turn(0), in_turn(1)
    near = lax.rem(lat + 1, 2)

    def prepare(k, f):
        mix_field(k, f)
        send_halo(k, f)

    def inputs_start(c):
        for f in range(2):
            in_copy(c, f).start()

    def inputs_wait(c):
        for f in range(2):
            in_copy(c, f).wait()

    inputs_wait(0)
    r_copy().wait()
    weights_start(early, 1)
    mix_field(0, early)
    pl.semaphore_wait(barrier, sum(present.astype(jnp.int32) for present, _ in neighbours))
    send_halo(0, early)
    for n in range(2, SLICES):
        weights_start(early, n)
    prepare(0, late)
    for c in range(2, chunks):
        inputs_start(c)
    first_block(early, near)
    for n in range(SLICES):
        weights_start(late, n)
    inputs_wait(1)
    prepare(1, early)
    prepare(1, late)
    for c in range(2, chunks):
        inputs_wait(c)

    @pl.loop(2, chunks)
    def _(k):
        mix(k)

    first_block(early, 1 - near)
    finish(0, early, False)

    @pl.loop(1, chunks - 1)
    def _(k):
        extrapolate_field(k, early, False)

    for n in range(SLICES):
        weights_wait(late, n)

    @pl.loop(0, chunks - 1)
    def _(k):
        extrapolate_field(k, late, False)

    def sent(k, last):
        for f in range(2):
            @pl.when(has_left)
            def _():
                halo_copy(k, 0, f).wait_send()

            @pl.when(has_right)
            def _():
                halo_copy(k, 1, f).wait_send()

        @pl.when(not_last)
        def _():
            depth_copy(k, 0, last).wait_send()

        @pl.when(not_first)
        def _():
            depth_copy(k, 1, last).wait_send()

    @pl.loop(chunks, steps - chunks + 1)
    def _(k):
        arrived(k - chunks, False)

        @pl.when(k >= ring)
        def _():
            sent(k - ring, False)

        mix(k)
        extrapolate(k - 1, False)

    @pl.loop(steps - chunks + 1, steps)
    def _(k):
        arrived(k - chunks, False)
        sent(k - ring, False)
        mix(k)
        extrapolate(k - 1, True)

    extrapolate(steps - 1, True)

    @pl.loop(steps - ring, steps - chunks)
    def _(k):
        sent(k, False)

    @pl.loop(steps - chunks, steps)
    def _(k):
        sent(k, True)
        arrived(k, True)


def store(down, up, down_out, up_out, sem):
    copies = [
        pltpu.make_async_copy(source, target, sem.at[f])
        for f, (source, target) in enumerate(((down, down_out), (up, up_out)))
    ]
    for copy in copies:
        copy.start()
    for copy in copies:
        copy.wait()


def solution(mesh):
    depths, lats = mesh.shape["depth"], mesh.shape["lat"]

    def on_device(down_state, up_state, reflectivity, w_down, w_up):
        _, columns, points = down_state.shape
        chunks = chunks_of(columns)
        rows = columns // chunks
        steps = TICKS * chunks
        window = w_down.shape[2]
        field = pltpu.VMEM(down_state.shape, jnp.bfloat16)
        landing = pl.BlockSpec(memory_space=pltpu.VMEM)
        anywhere = pl.BlockSpec(memory_space=pl.ANY)
        flops = 2 * 2 * TICKS * columns * points * window
        results = pl.pallas_call(
            functools.partial(kernel, depths, lats, chunks),
            out_shape=(field, field),
            in_specs=[anywhere] * 5,
            out_specs=(landing, landing),
            scratch_shapes=[
                pltpu.VMEM((steps, 2, rows, points), jnp.bfloat16),
                pltpu.VMEM((steps, 2, rows, points + 2 * HALO), jnp.bfloat16),
                pltpu.VMEM((steps, 2, rows, points), jnp.bfloat16),
                pltpu.VMEM((2, window, BLOCK), jnp.bfloat16),
                pltpu.VMEM((1, points), jnp.float32),
                pltpu.SemaphoreType.DMA((chunks, 2)),
                pltpu.SemaphoreType.DMA((2, SLICES)),
                pltpu.SemaphoreType.DMA,
                pltpu.SemaphoreType.DMA((2 * chunks, 2, 2)),
                pltpu.SemaphoreType.DMA((2 * chunks, 2, 2)),
                pltpu.SemaphoreType.DMA((2 * chunks, 2)),
                pltpu.SemaphoreType.DMA((2 * chunks, 2)),
            ],
            compiler_params=pltpu.CompilerParams(
                collective_id=0, has_side_effects=True, vmem_limit_bytes=VMEM_BYTES - 2 * 2 * down_state.size
            ),
            cost_estimate=pl.CostEstimate(
                flops=flops, bytes_accessed=4 * w_down.size * 2, transcendentals=0
            ),
        )(down_state, up_state, reflectivity, w_down, w_up)
        results = [pltpu.with_memory_space_constraint(result, pltpu.VMEM) for result in results]
        whole = jax.ShapeDtypeStruct(down_state.shape, jnp.bfloat16)
        return pl.pallas_call(
            store,
            out_shape=(whole, whole),
            in_specs=[landing] * 2,
            out_specs=(anywhere, anywhere),
            scratch_shapes=[pltpu.SemaphoreType.DMA((2,))],
            cost_estimate=pl.CostEstimate(
                flops=0, bytes_accessed=4 * 2 * down_state.size, transcendentals=0
            ),
        )(*results)

    in_specs = (
        P("depth", None, "lat"),
        P("depth", None, "lat"),
        P("depth", "lat"),
        P("depth", "lat", None, None),
        P("depth", "lat", None, None),
    )
    out_specs = (P("depth", None, "lat"), P("depth", None, "lat"))
    return jax.shard_map(
        on_device, mesh=mesh, in_specs=in_specs, out_specs=out_specs, check_vma=False
    )
```
